32 devices in a mesh: blk: 8 (over y, x, core), group: 4 (over z).
Axes of the slice: x: 2, y: 2, z: 4, core: 2. Of those that a mesh axis runs over, the one named last changes fastest.
Arguments:
- image_embed: bfloat16 [2048, 1152], P(('blk', 'group')), may hold values from -6 to 6
- caption_vectors: bfloat16 [16384, 1152], P(('blk', 'group')), may hold values from -6 to 6
- caption_counts: int32 [2048], replicated, may hold values from 1 to 8, as said below
- natural_log_multiplier: float32 [1], replicated, may hold values from 1.5 to 2.5
- match_odds_offset: float32 [1], replicated, may hold values from -6 to -4
Outputs:
- image_grad: float32 [2048, 1152], P(('blk', 'group'))
- caption_grad: float32 [16384, 1152], P(('blk', 'group'))
The draws below stay inside these ranges and needn't reach their ends.
Inputs may be any that keep to these rules, and one draw needn't show every extreme that they name: Images are numbered as in caption_counts, 64 to a device, devices in the order of blk then group. Local image k of the device with blk index b < 4 and group index g and local image k of the device with blk index b + 4 and group index g have counts that sum to 9. On at least one device all 64 images have 8 captions.
All inputs are finite; a program needn't handle non-finite values.
Results may differ from the reference program's by a relative error of at most 0.0028.
Values may be sent and summed in bfloat16 or wider, within the bound.
A program may use at most 64 MiB of HBM per device.

```python
import jax
import jax.numpy as jnp
from jax import lax

EMBED_WIDTH = 1152
NI_DEV = 64
CAP = 512
NI = 2048
CAPTION_SLOTS = 16384
N_BLK = 8
N_GROUP = 4
DEVICES = 32


def draw_caption_counts(key, part):
    half_blocks = N_BLK // 2
    level_key = jax.random.fold_in(key, 11)
    jitter_key = jax.random.fold_in(key, 12)
    flip_key = jax.random.fold_in(key, 13)
    full_key = jax.random.fold_in(key, 14)
    pair_level = jax.random.randint(level_key, (half_blocks, N_GROUP, 1), 1, 9)
    jitter = jax.random.randint(jitter_key, (half_blocks, N_GROUP, NI_DEV), -1, 2)
    lower_counts = jnp.clip(pair_level + jitter, 1, 8)
    full_pair = jax.random.randint(full_key, (), 0, half_blocks * N_GROUP)
    pair_number = jnp.arange(half_blocks * N_GROUP, dtype=jnp.int32).reshape(half_blocks, N_GROUP, 1)
    lower_counts = jnp.where(pair_number == full_pair, 8, lower_counts)
    flipped = jax.random.randint(flip_key, (half_blocks, N_GROUP, 1), 0, 2)
    lower_counts = jnp.where(flipped == 1, 9 - lower_counts, lower_counts)
    upper_counts = 9 - lower_counts
    return jnp.concatenate([lower_counts, upper_counts], axis=0).reshape(-1).astype(jnp.int32)


def centre_table(key):
    raw_centres = jax.random.normal(jax.random.fold_in(key, 21), (128, EMBED_WIDTH), jnp.float32)
    return raw_centres / jnp.sqrt(jnp.sum(raw_centres * raw_centres, axis=1, keepdims=True))


def image_clusters(key):
    return jax.random.randint(jax.random.fold_in(key, 22), (NI,), 0, 128).astype(jnp.int32)


def mixed_rows(base_key, salt, clusters, mix_low, mix_high, scale_low, scale_high):
    row_count = clusters.shape[0]
    row_key = jax.random.fold_in(base_key, salt)
    jitter_rows = jax.random.normal(jax.random.fold_in(row_key, 1), (row_count, EMBED_WIDTH), jnp.float32)
    jitter_rows = jitter_rows / jnp.sqrt(jnp.sum(jitter_rows * jitter_rows, axis=1, keepdims=True))
    mix_weight = jax.random.uniform(jax.random.fold_in(row_key, 2), (row_count, 1), jnp.float32, mix_low, mix_high)
    log_scale = jax.random.uniform(jax.random.fold_in(row_key, 3), (row_count, 1), jnp.float32, jnp.log(scale_low), jnp.log(scale_high))
    picked = jnp.take(centre_table(base_key), clusters, axis=0)
    return jnp.exp(log_scale) * (mix_weight * picked + jnp.sqrt(1.0 - mix_weight * mix_weight) * jitter_rows)


def draw_image_embed(key, part):
    clusters = image_clusters(key)
    values = mixed_rows(key, 23, clusters, 0.35, 0.85, 0.999, 1.001)
    return values.astype(jnp.bfloat16)


def draw_caption_vectors(key, part):
    counts = draw_caption_counts(key, part)
    per_device = counts.reshape(DEVICES, NI_DEV).astype(jnp.int32)
    running_end = jnp.cumsum(per_device, axis=1).astype(jnp.int32)
    position = jnp.arange(CAP, dtype=jnp.int32)
    local_index = jnp.sum((running_end[:, None, :] <= position[None, :, None]).astype(jnp.int32), axis=2).astype(jnp.int32)
    first_image = (jnp.arange(DEVICES, dtype=jnp.int32) * NI_DEV)[:, None]
    live_slots = position[None, :] < running_end[:, -1:]
    owners = jnp.where(live_slots, first_image + local_index, 0).reshape(-1).astype(jnp.int32)
    owner_clusters = jnp.take(image_clusters(key), owners)
    spare_clusters = jax.random.randint(jax.random.fold_in(key, 24), (CAPTION_SLOTS,), 0, 128).astype(jnp.int32)
    clusters = jnp.where(live_slots.reshape(-1), owner_clusters, spare_clusters).astype(jnp.int32)
    values = mixed_rows(key, 25, clusters, 0.35, 0.85, 0.999, 1.001)
    return values.astype(jnp.bfloat16)


def setup_inputs(seed: int = 0) -> dict:
    streams_of = jax.random.split(jax.random.key(seed), 6)
    image_embed = draw_image_embed(jax.random.fold_in(streams_of[5], 71), 0)
    caption_vectors = draw_caption_vectors(jax.random.fold_in(streams_of[5], 71), 0)
    caption_counts = draw_caption_counts(jax.random.fold_in(streams_of[5], 71), 0)
    natural_log_multiplier = jnp.clip(jax.random.uniform(streams_of[3], (1,), jnp.float32, 1.5, 2.5), 1.5, 2.5)
    match_odds_offset = jnp.clip(jax.random.uniform(streams_of[4], (1,), jnp.float32, -6.0, -4.0), -6.0, -4.0)
    return dict(image_embed=image_embed, caption_vectors=caption_vectors, caption_counts=caption_counts, natural_log_multiplier=natural_log_multiplier, match_odds_offset=match_odds_offset)


EPSILON = 1e-06

def normalize(embed_rows):
    values = embed_rows.astype(jnp.float32)
    inverse = lax.rsqrt(lax.optimization_barrier(jnp.sum(values * values, axis=1, keepdims=True)) + EPSILON)
    return (values * inverse, inverse)

def owner_table(caption_counts):
    per_device = caption_counts.reshape(DEVICES, NI_DEV).astype(jnp.int32)
    running_end = jnp.cumsum(per_device, axis=1).astype(jnp.int32)
    position = jnp.arange(CAP, dtype=jnp.int32)
    local_index = lax.optimization_barrier(jnp.sum((running_end[:, None, :] <= position[None, :, None]).astype(jnp.int32), axis=2)).astype(jnp.int32)
    first_image = (jnp.arange(DEVICES, dtype=jnp.int32) * NI_DEV)[:, None]
    present_entry_flags = position[None, :] < running_end[:, -1:]
    return jnp.where(present_entry_flags, first_image + local_index, -1).astype(jnp.int32)

def reference(image_embed, caption_vectors, caption_counts, natural_log_multiplier, match_odds_offset):
    image_unit, image_inverse = normalize(image_embed)
    caption_unit, caption_inverse = normalize(caption_vectors)
    image_low = image_unit.astype(jnp.bfloat16)
    caption_low = caption_unit.astype(jnp.bfloat16)
    owners = owner_table(caption_counts)
    odds_sharpness_factor = jnp.exp(natural_log_multiplier[0])
    image_ids = jnp.arange(NI, dtype=jnp.int32)
    picture_entry_extent = image_low.T

    def one_block(image_sum, inputs):
        tile_line_extent, block_owner = inputs
        similarity_matrix = odds_sharpness_factor * jnp.dot(tile_line_extent, picture_entry_extent, preferred_element_type=jnp.float32) + match_odds_offset[0]
        match_target_signs = jnp.where(block_owner[:, None] == image_ids[None, :], 1.0, -1.0)
        present_entry_flags = (block_owner >= 0)[:, None]
        oriented_similarity_gap = match_target_signs * similarity_matrix
        match_loss_factors = jnp.where(present_entry_flags, odds_sharpness_factor * (-match_target_signs * jax.nn.sigmoid(-oriented_similarity_gap)), 0.0).astype(jnp.bfloat16)
        caption_sum = jnp.dot(match_loss_factors, image_low, preferred_element_type=jnp.float32)
        image_sum = image_sum + jnp.dot(match_loss_factors.T, tile_line_extent, preferred_element_type=jnp.float32)
        return (image_sum, caption_sum)
    initial = jnp.zeros((NI, EMBED_WIDTH), jnp.float32)
    image_sum, caption_sum = lax.scan(one_block, initial, (caption_low.reshape(DEVICES, CAP, EMBED_WIDTH), owners))
    caption_sum = caption_sum.reshape(DEVICES * CAP, EMBED_WIDTH)
    image_grad = (image_sum - image_unit * lax.optimization_barrier(jnp.sum(image_unit * image_sum, axis=1, keepdims=True))) * image_inverse
    slot_live = (owners.reshape(-1) >= 0)[:, None]
    caption_grad = jnp.where(slot_live, (caption_sum - caption_unit * lax.optimization_barrier(jnp.sum(caption_unit * caption_sum, axis=1, keepdims=True))) * caption_inverse, 0.0)
    return (image_grad, caption_grad)
```

```python
import functools

import jax
import jax.numpy as jnp
from jax import lax
from jax.experimental import pallas as pl
from jax.experimental.pallas import tpu as pltpu
from jax.sharding import PartitionSpec as P

EPSILON = 1e-06
MESH = pl.DeviceIdType.MESH
ROWS = 256


def normalize(embed_rows):
    values = embed_rows.astype(jnp.float32)
    inverse = lax.rsqrt(jnp.sum(values * values, axis=1, keepdims=True) + EPSILON)
    return (values * inverse, inverse)


def flipped(index, mask):
    bit = 1
    while bit <= mask:
        if mask & bit:
            index = index + bit - 2 * bit * ((index // bit) % 2)
        bit *= 2
    return index


def kernel(
    chips, groups,
    image_ref, caption_ref, bounds_ref, totals_ref, scalars_ref,
    image_grad_ref, caption_grad_ref,
    images, captions, caption_inverse, caption_sum, own_partial, partial,
    out_partial, in_partial, out_sum, in_sum, out_caption, in_caption,
    line_send, line_recv, plane_send, plane_recv, part_send, part_recv,
    sum_send, sum_recv, pair_send, pair_recv,
):
    blk = lax.axis_index("blk")
    group = lax.axis_index("group")
    core = blk % 2
    chip = blk // 2
    image_count = image_ref.shape[0]
    slots = caption_ref.shape[0]
    columns = groups * image_count
    masks = sorted(range(1, chips), key=lambda m: (bin(m).count("1"), m))
    temperature = scalars_ref[0]
    bias = scalars_ref[1]

    def plane_peer(mask):
        return (flipped(chip, mask) * 2 + core, group)

    def line_peer(distance):
        return (blk, (group + distance) % groups)

    pair_peer = (chip * 2 + 1 - core, group)

    barrier = pltpu.get_barrier_semaphore()
    peers = [pair_peer]
    peers += [plane_peer(m) for m in masks]
    peers += [line_peer(d) for d in range(1, groups)]
    for peer in peers:
        pl.semaphore_signal(barrier, inc=1, device_id=peer, device_id_type=MESH)
    image_unit, image_inverse = normalize(image_ref[...])
    images[chip, group] = image_unit.astype(jnp.bfloat16)
    pl.semaphore_wait(barrier, len(peers))

    def remote(source, target, send, recv, peer):
        return pltpu.make_async_remote_copy(
            src_ref=source, dst_ref=target, send_sem=send, recv_sem=recv,
            device_id=peer, device_id_type=MESH,
        )

    def line_copy(d):
        here = images.at[chip, group]
        return remote(here, here, line_send.at[d - 1], line_recv.at[d - 1], line_peer(d))

    def plane_copy(mask, d):
        here = images.at[chip, (group - d + groups) % groups]
        return remote(
            here, here, plane_send.at[mask - 1, d], plane_recv.at[mask - 1, d], plane_peer(mask)
        )

    def part_copy(mask, unit):
        return remote(
            out_partial.at[mask - 1, unit], in_partial.at[mask - 1, unit],
            part_send.at[mask - 1, unit], part_recv.at[mask - 1, unit], plane_peer(mask),
        )

    def sum_copy(d):
        return remote(
            out_sum.at[d - 1], in_sum.at[d - 1], sum_send.at[d - 1], sum_recv.at[d - 1],
            line_peer(d),
        )

    near = [m for m in masks if bin(m).count("1") == 1]
    far = [m for m in masks if m not in near]
    for d in range(1, groups):
        line_copy(d).start()
    for m in masks:
        plane_copy(m, 0).start()

    step = min(slots, 128)

    @pl.loop(0, slots // step)
    def _(i):
        rows = pl.ds(pl.multiple_of(i * step, step), step)
        unit, inverse = normalize(caption_ref[rows, :])
        captions[0, rows, :] = unit.astype(jnp.bfloat16)
        caption_inverse[rows, :] = inverse

    caption_copy = remote(
        captions.at[0], captions.at[1], pair_send.at[0], pair_recv.at[0], pair_peer
    )
    caption_copy.start()
    for d in range(1, groups):
        line_copy(d).wait_recv()
        for m in near:
            plane_copy(m, d).start()
    for d in range(1, groups):
        for m in far:
            plane_copy(m, d).start()
    caption_copy.wait_recv()

    blocks = slots // ROWS

    def chunk(source_chip, target, own):
        target[...] = jnp.zeros_like(target)

        @pl.loop(0, 2 * blocks)
        def _(i):
            half = i // blocks
            offset = pl.multiple_of((i % blocks) * ROWS, ROWS)
            rows = pl.ds(offset, ROWS)
            block = captions[half, rows, :]
            picked = images[source_chip].reshape(columns, -1)
            scores = temperature * lax.dot_general(
                block, picked, (((1,), (1,)), ((), ())), preferred_element_type=jnp.float32
            ) + bias
            position = offset + lax.broadcasted_iota(jnp.int32, scores.shape, 0)
            chance = 1.0 / (1.0 + jnp.exp(-scores))
            if own:
                shifted = position + half * slots
                match = (shifted >= bounds_ref[0:1, :]) & (shifted < bounds_ref[1:2, :])
                chance = jnp.where(match, -1.0 / (1.0 + jnp.exp(scores)), chance)
            weight = jnp.where(position < totals_ref[half], temperature * chance, 0.0)
            weight = weight.astype(jnp.bfloat16)
            gained = jnp.dot(weight, picked, preferred_element_type=jnp.float32)
            if own:
                caption_sum[half, rows, :] = gained
            else:
                caption_sum[half, rows, :] += gained
            target[...] += lax.dot_general(
                weight, block, (((0,), (0,)), ((), ())), preferred_element_type=jnp.float32
            )

    chunk(chip, own_partial, True)
    for m in masks:
        for d in range(groups):
            plane_copy(m, d).wait_recv()
        chunk(flipped(chip, m), partial, False)
        for unit in range(groups):
            rows = slice(unit * image_count, (unit + 1) * image_count)
            out_partial[m - 1, unit] = partial[rows, :].astype(jnp.bfloat16)
            part_copy(m, unit).start()

    out_caption[...] = caption_sum[1].astype(jnp.bfloat16)
    back_copy = remote(out_caption, in_caption, pair_send.at[1], pair_recv.at[1], pair_peer)
    back_copy.start()

    def column_total(unit):
        rows = pl.ds(pl.multiple_of(unit * image_count, image_count), image_count)
        total = own_partial[rows, :]
        for m in masks:
            part_copy(m, unit).wait_recv()
            total = total + in_partial[m - 1, unit].astype(jnp.float32)
        return total

    back_copy.wait_recv()

    @pl.loop(0, slots // step)
    def _(i):
        offset = pl.multiple_of(i * step, step)
        rows = pl.ds(offset, step)
        inverse = caption_inverse[rows, :]
        unit = caption_ref[rows, :].astype(jnp.float32) * inverse
        total = caption_sum[0, rows, :] + in_caption[rows, :].astype(jnp.float32)
        grad = (total - unit * jnp.sum(unit * total, axis=1, keepdims=True)) * inverse
        position = offset + lax.broadcasted_iota(jnp.int32, grad.shape, 0)
        caption_grad_ref[rows, :] = jnp.where(position < totals_ref[0], grad, 0.0)

    for d in range(1, groups):
        out_sum[d - 1] = column_total((group + d) % groups).astype(jnp.bfloat16)
        sum_copy(d).start()
    image_sum = column_total(group)
    for d in range(1, groups):
        sum_copy(d).wait_recv()
        image_sum = image_sum + in_sum[d - 1].astype(jnp.float32)
    image_unit, image_inverse = normalize(image_ref[...])
    image_grad_ref[...] = (
        image_sum - image_unit * jnp.sum(image_unit * image_sum, axis=1, keepdims=True)
    ) * image_inverse

    caption_copy.wait_send()
    back_copy.wait_send()
    for d in range(1, groups):
        line_copy(d).wait_send()
        sum_copy(d).wait_send()
    for m in masks:
        for d in range(groups):
            plane_copy(m, d).wait_send()
            part_copy(m, d).wait_send()


def shards(image_embed, caption_vectors, caption_counts, natural_log_multiplier, match_odds_offset):
    image_count, width = image_embed.shape
    slots = caption_vectors.shape[0]
    chips = lax.axis_size("blk") // 2
    groups = lax.axis_size("group")
    blk = lax.axis_index("blk")
    group = lax.axis_index("group")
    scalars = jnp.concatenate([jnp.exp(natural_log_multiplier), match_odds_offset])

    by_device = caption_counts.reshape(-1, image_count)
    own = lax.dynamic_index_in_dim(by_device, blk * groups + group, 0, keepdims=False)
    pair = lax.dynamic_index_in_dim(
        by_device, (blk + 1 - 2 * (blk % 2)) * groups + group, 0, keepdims=False
    )
    totals = jnp.stack([jnp.sum(own), jnp.sum(pair)])
    index = jnp.arange(image_count)
    ends = jnp.sum(jnp.where(index[:, None] <= index[None, :], own[:, None], 0), axis=0)
    bounds = jnp.stack([ends - own, ends])
    mine = jnp.arange(groups * image_count) // image_count == group
    bounds = jnp.where(mine[None, :], jnp.tile(bounds, (1, groups)), 4 * slots)

    vmem = pl.BlockSpec(memory_space=pltpu.VMEM)
    smem = pl.BlockSpec(memory_space=pltpu.SMEM)
    low, full = jnp.bfloat16, jnp.float32
    dma = pltpu.SemaphoreType.DMA
    columns = groups * image_count
    return pl.pallas_call(
        functools.partial(kernel, chips, groups),
        out_shape=(
            jax.ShapeDtypeStruct((image_count, width), full),
            jax.ShapeDtypeStruct((slots, width), full),
        ),
        in_specs=[vmem, vmem, vmem, smem, smem],
        out_specs=(vmem, vmem),
        scratch_shapes=[
            pltpu.VMEM((chips, groups, image_count, width), low),
            pltpu.VMEM((2, slots, width), low),
            pltpu.VMEM((slots, 1), full),
            pltpu.VMEM((2, slots, width), full),
            pltpu.VMEM((columns, width), full),
            pltpu.VMEM((columns, width), full),
            pltpu.VMEM((chips - 1, groups, image_count, width), low),
            pltpu.VMEM((chips - 1, groups, image_count, width), low),
            pltpu.VMEM((groups - 1, image_count, width), low),
            pltpu.VMEM((groups - 1, image_count, width), low),
            pltpu.VMEM((slots, width), low),
            pltpu.VMEM((slots, width), low),
            dma((groups - 1,)), dma((groups - 1,)),
            dma((chips - 1, groups)), dma((chips - 1, groups)),
            dma((chips - 1, groups)), dma((chips - 1, groups)),
            dma((groups - 1,)), dma((groups - 1,)),
            dma((2,)), dma((2,)),
        ],
        compiler_params=pltpu.CompilerParams(collective_id=0, has_side_effects=True),
    )(image_embed, caption_vectors, bounds, totals, scalars)


def solution(mesh):
    placed = (P(("blk", "group"), None), P(("blk", "group"), None), P(), P(), P())
    return jax.shard_map(
        shards,
        mesh=mesh,
        in_specs=placed,
        out_specs=(P(("blk", "group"), None), P(("blk", "group"), None)),
        check_vma=False,
    )
```

```python
import functools

import jax
import jax.numpy as jnp
from jax import lax
from jax.experimental import pallas as pl
from jax.experimental.pallas import tpu as pltpu
from jax.sharding import PartitionSpec as P

EPSILON = 1e-06
MESH = pl.DeviceIdType.MESH
ROWS = 256


def normalize(embed_rows):
    values = embed_rows.astype(jnp.float32)
    inverse = lax.rsqrt(jnp.sum(values * values, axis=1, keepdims=True) + EPSILON)
    return (values * inverse, inverse)


def flipped(index, mask):
    bit = 1
    while bit <= mask:
        if mask & bit:
            index = index + bit - 2 * bit * ((index // bit) % 2)
        bit *= 2
    return index


def kernel(
    chips, groups,
    image_ref, caption_ref, bounds_ref, totals_ref, scalars_ref,
    image_grad_ref, caption_grad_ref,
    images, captions, caption_inverse, caption_sum, own_partial, partial,
    out_partial, in_partial, out_sum, in_sum, out_caption, in_caption,
    line_send, line_recv, plane_send, plane_recv, part_send, part_recv,
    sum_send, sum_recv, pair_send, pair_recv,
):
    blk = lax.axis_index("blk")
    group = lax.axis_index("group")
    core = blk % 2
    chip = blk // 2
    image_count = image_ref.shape[0]
    slots = caption_ref.shape[0]
    columns = groups * image_count
    masks = sorted(range(1, chips), key=lambda m: (bin(m).count("1"), m))
    temperature = scalars_ref[0]
    bias = scalars_ref[1]

    def plane_peer(mask):
        return (flipped(chip, mask) * 2 + core, group)

    def line_peer(distance):
        return (blk, (group + distance) % groups)

    pair_peer = (chip * 2 + 1 - core, group)

    barrier = pltpu.get_barrier_semaphore()
    peers = [pair_peer]
    peers += [plane_peer(m) for m in masks]
    peers += [line_peer(d) for d in range(1, groups)]
    for peer in peers:
        pl.semaphore_signal(barrier, inc=1, device_id=peer, device_id_type=MESH)
    image_unit, image_inverse = normalize(image_ref[...])
    images[chip, group] = image_unit.astype(jnp.bfloat16)
    pl.semaphore_wait(barrier, len(peers))

    def remote(source, target, send, recv, peer):
        return pltpu.make_async_remote_copy(
            src_ref=source, dst_ref=target, send_sem=send, recv_sem=recv,
            device_id=peer, device_id_type=MESH,
        )

    def line_copy(d):
        here = images.at[chip, group]
        return remote(here, here, line_send.at[d - 1], line_recv.at[d - 1], line_peer(d))

    near = [m for m in masks if bin(m).count("1") == 1]
    far = [m for m in masks if m not in near]

    def first_hop(mask, index):
        bits = [b for b in near if b & mask]
        return bits[index % len(bits)]

    def plane_copy(mask, d):
        first = 0 if mask in near else first_hop(mask, d)
        here = images.at[flipped(chip, first), (group - d + groups) % groups]
        return remote(
            here, here, plane_send.at[mask - 1, d], plane_recv.at[mask - 1, d],
            plane_peer(mask - first),
        )

    def relayed(mask):
        return bin(mask).count("1") == 2

    def joining(mask, unit):
        return [
            m for m in far if relayed(m) and mask in near and m - first_hop(m, unit) == mask
        ]

    def part_copy(mask, unit):
        first = first_hop(mask, unit) if relayed(mask) else mask
        return remote(
            out_partial.at[mask - 1, unit], in_partial.at[mask - 1, unit],
            part_send.at[mask - 1, unit], part_recv.at[mask - 1, unit], plane_peer(first),
        )

    def sum_copy(d):
        return remote(
            out_sum.at[d - 1], in_sum.at[d - 1], sum_send.at[d - 1], sum_recv.at[d - 1],
            line_peer(d),
        )

    for d in range(1, groups):
        line_copy(d).start()
    for m in near:
        plane_copy(m, 0).start()

    step = min(slots, 128)

    @pl.loop(0, slots // step)
    def _(i):
        rows = pl.ds(pl.multiple_of(i * step, step), step)
        unit, inverse = normalize(caption_ref[rows, :])
        captions[0, rows, :] = unit.astype(jnp.bfloat16)
        caption_inverse[rows, :] = inverse

    caption_copy = remote(
        captions.at[0], captions.at[1], pair_send.at[0], pair_recv.at[0], pair_peer
    )
    caption_copy.start()
    for d in range(1, groups):
        line_copy(d).wait_recv()
        for m in near:
            plane_copy(m, d).start()
    caption_copy.wait_recv()

    blocks = slots // ROWS

    def chunk(source_chip, target, own):
        target[...] = jnp.zeros_like(target)

        @pl.loop(0, 2 * blocks)
        def _(i):
            half = i // blocks
            offset = pl.multiple_of((i % blocks) * ROWS, ROWS)
            rows = pl.ds(offset, ROWS)
            block = captions[half, rows, :]
            picked = images[source_chip].reshape(columns, -1)
            scores = temperature * lax.dot_general(
                block, picked, (((1,), (1,)), ((), ())), preferred_element_type=jnp.float32
            ) + bias
            position = offset + lax.broadcasted_iota(jnp.int32, scores.shape, 0)
            chance = 1.0 / (1.0 + jnp.exp(-scores))
            if own:
                shifted = position + half * slots
                match = (shifted >= bounds_ref[0:1, :]) & (shifted < bounds_ref[1:2, :])
                chance = jnp.where(match, -1.0 / (1.0 + jnp.exp(scores)), chance)
            weight = jnp.where(position < totals_ref[half], temperature * chance, 0.0)
            weight = weight.astype(jnp.bfloat16)
            gained = jnp.dot(weight, picked, preferred_element_type=jnp.float32)
            if own:
                caption_sum[half, rows, :] = gained
            else:
                caption_sum[half, rows, :] += gained
            target[...] += lax.dot_general(
                weight, block, (((0,), (0,)), ((), ())), preferred_element_type=jnp.float32
            )

    chunk(chip, own_partial, True)
    for d in range(groups):
        for m in near:
            plane_copy(m, d).wait_recv()
        for m in far:
            plane_copy(m, d).start()
    for m in masks:
        for d in range(groups if m in far else 0):
            plane_copy(m, d).wait_recv()
        chunk(flipped(chip, m), partial, False)
        for unit in range(groups):
            rows = slice(unit * image_count, (unit + 1) * image_count)
            out_partial[m - 1, unit] = partial[rows, :].astype(jnp.bfloat16)
            if not joining(m, unit):
                part_copy(m, unit).start()

    for unit in range(groups):
        for m in near:
            sources = joining(m, unit)
            if sources:
                total = out_partial[m - 1, unit].astype(jnp.float32)
                for source in sources:
                    part_copy(source, unit).wait_recv()
                    total = total + in_partial[source - 1, unit].astype(jnp.float32)
                out_partial[m - 1, unit] = total.astype(jnp.bfloat16)
                part_copy(m, unit).start()

    out_caption[...] = caption_sum[1].astype(jnp.bfloat16)
    back_copy = remote(out_caption, in_caption, pair_send.at[1], pair_recv.at[1], pair_peer)
    back_copy.start()

    def column_total(unit):
        rows = pl.ds(pl.multiple_of(unit * image_count, image_count), image_count)
        total = own_partial[rows, :]
        for m in masks:
            if relayed(m):
                continue
            part_copy(m, unit).wait_recv()
            total = total + in_partial[m - 1, unit].astype(jnp.float32)
        return total

    back_copy.wait_recv()

    @pl.loop(0, slots // step)
    def _(i):
        offset = pl.multiple_of(i * step, step)
        rows = pl.ds(offset, step)
        inverse = caption_inverse[rows, :]
        unit = caption_ref[rows, :].astype(jnp.float32) * inverse
        total = caption_sum[0, rows, :] + in_caption[rows, :].astype(jnp.float32)
        grad = (total - unit * jnp.sum(unit * total, axis=1, keepdims=True)) * inverse
        position = offset + lax.broadcasted_iota(jnp.int32, grad.shape, 0)
        caption_grad_ref[rows, :] = jnp.where(position < totals_ref[0], grad, 0.0)

    for d in range(1, groups):
        out_sum[d - 1] = column_total((group + d) % groups).astype(jnp.bfloat16)
        sum_copy(d).start()
    image_sum = column_total(group)
    for d in range(1, groups):
        sum_copy(d).wait_recv()
        image_sum = image_sum + in_sum[d - 1].astype(jnp.float32)
    image_unit, image_inverse = normalize(image_ref[...])
    image_grad_ref[...] = (
        image_sum - image_unit * jnp.sum(image_unit * image_sum, axis=1, keepdims=True)
    ) * image_inverse

    caption_copy.wait_send()
    back_copy.wait_send()
    for d in range(1, groups):
        line_copy(d).wait_send()
        sum_copy(d).wait_send()
    for m in masks:
        for d in range(groups):
            plane_copy(m, d).wait_send()
            part_copy(m, d).wait_send()


def shards(image_embed, caption_vectors, caption_counts, natural_log_multiplier, match_odds_offset):
    image_count, width = image_embed.shape
    slots = caption_vectors.shape[0]
    chips = lax.axis_size("blk") // 2
    groups = lax.axis_size("group")
    blk = lax.axis_index("blk")
    group = lax.axis_index("group")
    scalars = jnp.concatenate([jnp.exp(natural_log_multiplier), match_odds_offset])

    by_device = caption_counts.reshape(-1, image_count)
    own = lax.dynamic_index_in_dim(by_device, blk * groups + group, 0, keepdims=False)
    pair = lax.dynamic_index_in_dim(
        by_device, (blk + 1 - 2 * (blk % 2)) * groups + group, 0, keepdims=False
    )
    totals = jnp.stack([jnp.sum(own), jnp.sum(pair)])
    index = jnp.arange(image_count)
    ends = jnp.sum(jnp.where(index[:, None] <= index[None, :], own[:, None], 0), axis=0)
    bounds = jnp.stack([ends - own, ends])
    mine = jnp.arange(groups * image_count) // image_count == group
    bounds = jnp.where(mine[None, :], jnp.tile(bounds, (1, groups)), 4 * slots)

    vmem = pl.BlockSpec(memory_space=pltpu.VMEM)
    smem = pl.BlockSpec(memory_space=pltpu.SMEM)
    low, full = jnp.bfloat16, jnp.float32
    dma = pltpu.SemaphoreType.DMA
    columns = groups * image_count
    return pl.pallas_call(
        functools.partial(kernel, chips, groups),
        out_shape=(
            jax.ShapeDtypeStruct((image_count, width), full),
            jax.ShapeDtypeStruct((slots, width), full),
        ),
        in_specs=[vmem, vmem, vmem, smem, smem],
        out_specs=(vmem, vmem),
        scratch_shapes=[
            pltpu.VMEM((chips, groups, image_count, width), low),
            pltpu.VMEM((2, slots, width), low),
            pltpu.VMEM((slots, 1), full),
            pltpu.VMEM((2, slots, width), full),
            pltpu.VMEM((columns, width), full),
            pltpu.VMEM((columns, width), full),
            pltpu.VMEM((chips - 1, groups, image_count, width), low),
            pltpu.VMEM((chips - 1, groups, image_count, width), low),
            pltpu.VMEM((groups - 1, image_count, width), low),
            pltpu.VMEM((groups - 1, image_count, width), low),
            pltpu.VMEM((slots, width), low),
            pltpu.VMEM((slots, width), low),
            dma((groups - 1,)), dma((groups - 1,)),
            dma((chips - 1, groups)), dma((chips - 1, groups)),
            dma((chips - 1, groups)), dma((chips - 1, groups)),
            dma((groups - 1,)), dma((groups - 1,)),
            dma((2,)), dma((2,)),
        ],
        compiler_params=pltpu.CompilerParams(collective_id=0, has_side_effects=True),
    )(image_embed, caption_vectors, bounds, totals, scalars)


def solution(mesh):
    placed = (P(("blk", "group"), None), P(("blk", "group"), None), P(), P(), P())
    return jax.shard_map(
        shards,
        mesh=mesh,
        in_specs=placed,
        out_specs=(P(("blk", "group"), None), P(("blk", "group"), None)),
        check_vma=False,
    )
```
